8 devices in a mesh: stage: 2 (over z, y), expert: 4 (over x, core).
Axes of the slice: x: 2, y: 2, z: 1, core: 2. Of those that a mesh axis runs over, the one named last changes fastest.
Arguments:
- w_gate: bfloat16 [2, 16, 2560, 1536], P('stage', 'expert')
- w_up: bfloat16 [2, 16, 2560, 1536], P('stage', 'expert')
- w_down: bfloat16 [2, 16, 1536, 2560], P('stage', 'expert')
- x: bfloat16 [2048, 2560], P(('stage', 'expert'))
- expert_ids: int32 [2, 2048, 6], P(None, ('stage', 'expert'))
- gates: float32 [2, 2048, 6], P(None, ('stage', 'expert'))
Outputs:
- output 1: bfloat16 [2, 16, 2560, 3072], P(None, ('stage', 'expert'))
- output 2: bfloat16 [2, 16, 1536, 2560], P(None, ('stage', 'expert'))
- output 3: float32 [2, 2048, 2560], P(None, ('stage', 'expert'))
All inputs are finite; a program needn't handle non-finite values.
Results may differ from the reference program's by a relative error of at most 0.001.
Values are sent between devices in bfloat16 or wider.
A program may use at most 1 GiB of HBM per device.

```python
import jax
import jax.numpy as jnp
from jax import lax

D = 2560
FF = 1536
TOP = 6
LAYERS = 2
EXPERTS = 16
DEVICES = 8
TOK_DEV = 256

TOKENS = DEVICES * TOK_DEV
CAPACITY = 3 * TOK_DEV * TOP // (2 * EXPERTS)
NORM_EPS = 1e-6


def draw_routes(key):
    mean_load = TOK_DEV * TOP // EXPERTS
    half_load = mean_load // 2
    blocks = LAYERS * DEVICES
    key_shift, key_expert, key_token = jax.random.split(key, 3)
    shifts = jax.random.randint(key_shift, (blocks, EXPERTS // 2), 0, half_load + 1)
    shifts = shifts.at[:, 0].set(half_load)
    counts = jnp.stack([mean_load + shifts, mean_load - shifts], axis=-1).reshape(blocks, EXPERTS)
    run_ends = jnp.cumsum(counts, axis=-1)
    entry = jnp.arange(TOK_DEV * TOP)
    virtual = jnp.sum((entry[None, :, None] >= run_ends[:, None, :]).astype(jnp.int32), axis=-1)
    expert_perm = jax.vmap(lambda sub_key: jax.random.permutation(sub_key, EXPERTS))(jax.random.split(key_expert, blocks))
    labels = jax.vmap(lambda table, index: table[index])(expert_perm, virtual)
    labels = jnp.transpose(labels.reshape(blocks, TOP, TOK_DEV), (0, 2, 1))
    token_perm = jax.vmap(lambda sub_key: jax.random.permutation(sub_key, TOK_DEV))(jax.random.split(key_token, blocks))
    routed = jax.vmap(lambda table, index: table[index])(labels, token_perm)
    return routed.reshape(LAYERS, TOKENS, TOP).astype(jnp.int32)


def setup_inputs(seed: int = 0) -> dict:
    key = jax.random.key(seed)
    key_gate, key_up, key_down, key_x, key_mix, key_route = jax.random.split(key, 6)
    w_gate = (jax.random.normal(key_gate, (LAYERS, EXPERTS, D, FF), jnp.float32) * D ** -0.5).astype(jnp.bfloat16)
    w_up = (jax.random.normal(key_up, (LAYERS, EXPERTS, D, FF), jnp.float32) * D ** -0.5).astype(jnp.bfloat16)
    w_down = (jax.random.normal(key_down, (LAYERS, EXPERTS, FF, D), jnp.float32) * FF ** -0.5).astype(jnp.bfloat16)
    x = jax.random.normal(key_x, (TOKENS, D), jnp.float32).astype(jnp.bfloat16)
    gates = jax.nn.softmax(jax.random.normal(key_mix, (LAYERS, TOKENS, TOP), jnp.float32), axis=-1)
    expert_ids = draw_routes(key_route)
    return {"w_gate": w_gate, "w_up": w_up, "w_down": w_down, "x": x, "expert_ids": expert_ids, "gates": gates}


def expert_layer(hidden, layer_in):
    layer_w13, layer_down, layer_ids, layer_mix = layer_in
    normed = (hidden * lax.rsqrt(jnp.mean(hidden * hidden, axis=-1, keepdims=True) + NORM_EPS)).astype(jnp.bfloat16)
    flat_ids = layer_ids.reshape(-1)
    onehot = (flat_ids[:, None] == jnp.arange(EXPERTS)[None, :]).astype(jnp.int32)
    pair_rank = jnp.sum(onehot * jnp.cumsum(onehot, axis=0), axis=-1) - 1
    rows_per_expert = DEVICES * CAPACITY
    slot_pos = flat_ids * rows_per_expert + pair_rank
    pair_tok = jnp.arange(TOKENS * TOP) // TOP
    buffer = jnp.zeros((EXPERTS * rows_per_expert, D), jnp.bfloat16).at[slot_pos].set(normed[pair_tok])
    buffer = buffer.reshape(EXPERTS, rows_per_expert, D).astype(jnp.float32)
    projected = jnp.einsum("erd,edg->erg", buffer, layer_w13.astype(jnp.float32))
    activated = (jax.nn.silu(projected[..., :FF]) * projected[..., FF:]).astype(jnp.bfloat16)
    expert_out = jnp.einsum("erf,efd->erd", activated.astype(jnp.float32), layer_down.astype(jnp.float32)).astype(jnp.bfloat16)
    picked = expert_out.reshape(EXPERTS * rows_per_expert, D)[slot_pos].astype(jnp.float32).reshape(TOKENS, TOP, D)
    new_hidden = hidden + jnp.sum(layer_mix[..., None] * picked, axis=1)
    return new_hidden, new_hidden


def reference(w_gate, w_up, w_down, x, expert_ids, gates):
    w13 = jnp.concatenate([w_gate, w_up], axis=-1)
    _, hiddens = lax.scan(expert_layer, x.astype(jnp.float32), (w13, w_down, expert_ids, gates))
    return w13, w_down, hiddens
```

```python
import functools

import jax
import jax.numpy as jnp
from jax import lax
from jax.experimental import pallas as pl
from jax.experimental.pallas import tpu as pltpu
from jax.sharding import PartitionSpec as P


NORM_EPS = 1e-6
FLAT = ("stage", "expert")
W13_CHUNKS = 4
DOWN_CHUNKS = 2


def norm_rows(hidden):
    return (hidden * lax.rsqrt(jnp.mean(hidden * hidden, axis=-1, keepdims=True) + NORM_EPS)).astype(jnp.bfloat16)


def copy_through(moves):
    for loads, _ in moves:
        for cp in loads:
            cp.start()
    for loads, store in moves:
        for cp in loads:
            cp.wait()
        store.start()
    for _, store in moves:
        store.wait()


def pick_w13_body(row_start, n, meta_ref, gate_ref, up_ref, out_ref, buf, sem_in, sem_out):
    exp_dev, rows, width = out_ref.shape
    half = width // 2
    tile = rows // n
    moves = []
    for e in range(exp_dev):
        for i in range(n):
            k = e * n + i
            src = pl.ds(row_start + i * tile, tile)
            exp = meta_ref[2] * exp_dev + e
            loads = [pltpu.make_async_copy(gate_ref.at[exp, src], buf.at[k, :, pl.ds(0, half)], sem_in.at[k, 0]),
                     pltpu.make_async_copy(up_ref.at[exp, src], buf.at[k, :, pl.ds(half, half)], sem_in.at[k, 1])]
            moves.append((loads, pltpu.make_async_copy(buf.at[k], out_ref.at[e, pl.ds(i * tile, tile)], sem_out.at[k])))
    copy_through(moves)


def pick_down_body(row_start, n, meta_ref, down_ref, out_ref, buf, sem_in, sem_out):
    exp_dev, rows, _ = out_ref.shape
    tile = rows // n
    moves = []
    for e in range(exp_dev):
        for i in range(n):
            k = e * n + i
            src = pl.ds(row_start + i * tile, tile)
            loads = [pltpu.make_async_copy(down_ref.at[meta_ref[2] * exp_dev + e, src], buf.at[k], sem_in.at[k, 0])]
            moves.append((loads, pltpu.make_async_copy(buf.at[k], out_ref.at[e, pl.ds(i * tile, tile)], sem_out.at[k])))
    copy_through(moves)


def place_body(row_start, n, meta_ref, landed_ref, own_ref, *rest):
    out_ref, buf, sem_in, sem_out = rest[-4:]
    exp_dev, rows, _ = landed_ref.shape
    tile = rows // n

    def moves_from(src_ref):
        moves = []
        for e in range(exp_dev):
            for i in range(n):
                k = e * n + i
                loads = [pltpu.make_async_copy(src_ref.at[e, pl.ds(i * tile, tile)], buf.at[k], sem_in.at[k])]
                moves.append((loads, pltpu.make_async_copy(buf.at[k], out_ref.at[meta_ref[0], e, pl.ds(row_start + i * tile, tile)], sem_out.at[k])))
        return moves

    pl.when(meta_ref[1] == 0)(lambda: copy_through(moves_from(landed_ref)))
    pl.when(meta_ref[1] != 0)(lambda: copy_through(moves_from(own_ref)))


HBM_SPEC = pl.BlockSpec(memory_space=pl.ANY)
SMEM_SPEC = pl.BlockSpec(memory_space=pltpu.SMEM)
COPY_COST = pl.CostEstimate(flops=5_000_000_000, bytes_accessed=16_000_000, transcendentals=0)
PIECES = 2


def pick(body, meta, sources, exp_dev, row_start, rows, width):
    dtype = sources[0].dtype
    n = PIECES
    return pl.pallas_call(
        functools.partial(body, row_start, n),
        out_shape=jax.ShapeDtypeStruct((exp_dev, rows, width), dtype),
        in_specs=[SMEM_SPEC] + [HBM_SPEC] * len(sources),
        out_specs=HBM_SPEC,
        scratch_shapes=[pltpu.VMEM((exp_dev * n, rows // n, width), dtype), pltpu.SemaphoreType.DMA((exp_dev * n, 2)), pltpu.SemaphoreType.DMA((exp_dev * n,))],
        cost_estimate=COPY_COST,
    )(meta, *sources)


def place(buffer, landed, own, meta, out_shape, row_start):
    exp_dev, rows, width = landed.shape
    n = PIECES
    args = [meta, landed, own] + ([] if buffer is None else [buffer])
    return pl.pallas_call(
        functools.partial(place_body, row_start, n),
        out_shape=jax.ShapeDtypeStruct(out_shape, landed.dtype),
        in_specs=[SMEM_SPEC] + [HBM_SPEC] * (len(args) - 1),
        out_specs=HBM_SPEC,
        scratch_shapes=[pltpu.VMEM((exp_dev * n, rows // n, width), landed.dtype), pltpu.SemaphoreType.DMA((exp_dev * n,)), pltpu.SemaphoreType.DMA((exp_dev * n,))],
        input_output_aliases={} if buffer is None else {3: 0},
        cost_estimate=COPY_COST,
    )(*args)


def round_meta(round_idx, n_stage, n_group):
    stage_idx = lax.axis_index("stage")
    group = lax.axis_index("expert")
    flat_idx = stage_idx * n_group + group
    piece = (stage_idx + round_idx) % n_stage
    is_self = group * n_stage + piece == flat_idx
    return jnp.stack([(flat_idx % n_stage - round_idx) % n_stage, is_self.astype(jnp.int32), piece]).astype(jnp.int32)


def send_round(round_idx, meta, gate_loc, up_loc, down_loc, n_stage, n_group):
    exp_dev = gate_loc.shape[0] // n_stage
    model_width, expert_width = gate_loc.shape[1:]
    pairs = [(s * n_group + g, g * n_stage + (s + round_idx) % n_stage) for s in range(n_stage) for g in range(n_group)]
    pairs = [p for p in pairs if p[0] != p[1]]
    chunks = []
    for kind, total, parts, width, body, sources in (
        ("w13", model_width, W13_CHUNKS, 2 * expert_width, pick_w13_body, (gate_loc, up_loc)),
        ("down", expert_width, DOWN_CHUNKS, model_width, pick_down_body, (down_loc,)),
    ):
        rows = total // parts
        for c in range(parts):
            idx = round_idx * (W13_CHUNKS + DOWN_CHUNKS) + len(chunks)
            own = pick(body, meta, sources, exp_dev, c * rows, rows, width)
            landed = lax.ppermute(own, FLAT, pairs)
            chunks.append((idx, kind, c * rows, own, landed))
    return chunks


def moe_body(layer_idx, dims, u_ref, mix_ref, gate_ref, up_ref, down_ref, parts_ref, stage_ref, tok, gbuf, ubuf, dbuf, act, acc, xbuf, xown, wcol, ld_sem, out_sem, g_sem, u_sem, d_sem, own_ss, own_rs, tok_ss, tok_rs, x_ss, x_rs, sum_ss, parts_rs):
    n_group, rows, width, ff, n_exp = dims
    block = 2 * rows
    g_tile = gbuf.shape[2]
    d_tile = dbuf.shape[2]
    g_steps = ff // g_tile
    d_steps = width // d_tile
    last = 2 * n_group - 1
    flat = lax.axis_index("stage") * n_group + lax.axis_index("expert")
    role = flat if layer_idx == 0 else last - flat
    chip = role // 2
    core = role % 2
    partner_role = 2 * chip + 1 - core

    def device(r):
        f = r if layer_idx == 0 else last - r
        return (f // n_group, f % n_group)

    def remote(src, dst, ss, rs, target):
        return pltpu.make_async_remote_copy(src_ref=src, dst_ref=dst, send_sem=ss, recv_sem=rs, device_id=device(target), device_id_type=pl.DeviceIdType.MESH)

    def tok_copy(b, target, kind):
        return remote(tok.at[b], tok.at[b], tok_ss.at[kind, b], tok_rs.at[b], target)

    def on(r, fn):
        pl.when(role == r)(fn)

    own_rows = pl.ds(pl.multiple_of(core * rows, rows), rows)
    other_rows = pl.ds(pl.multiple_of((1 - core) * rows, rows), rows)
    load_own = pltpu.make_async_copy(u_ref, tok.at[chip, own_rows], ld_sem)
    load_own.start()

    def g_copy(q):
        e, j, b = (q // g_steps) % n_exp, q % g_steps, q % 2
        cols = pl.ds(pl.multiple_of(j * g_tile, g_tile), g_tile)
        return (pltpu.make_async_copy(gate_ref.at[e, :, cols], gbuf.at[b], g_sem.at[b]),
                pltpu.make_async_copy(up_ref.at[e, :, cols], ubuf.at[b], u_sem.at[b]))

    def d_copy(p):
        e, n, b = (p // d_steps) % n_exp, p % d_steps, p % 2
        cols = pl.ds(pl.multiple_of(n * d_tile, d_tile), d_tile)
        return pltpu.make_async_copy(down_ref.at[e, :, cols], dbuf.at[b], d_sem.at[b])

    g_total = 4 * n_exp * g_steps
    d_total = 4 * n_exp * d_steps

    @pl.when(chip < 2)
    def _():
        for c in g_copy(0):
            c.start()
        d_copy(0).start()

    load_own.wait()
    own_copy = remote(tok.at[chip, own_rows], tok.at[chip, own_rows], own_ss, own_rs, partner_role)
    own_copy.start()
    own_copy.wait_recv()
    on(0, lambda: tok_copy(0, 2, 0).start())
    on(3, lambda: tok_copy(1, 1, 0).start())
    on(5, lambda: tok_copy(2, 0, 0).start())
    on(4, lambda: tok_copy(2, 3, 0).start())
    on(7, lambda: tok_copy(3, 1, 0).start())

    def x_copy(slot):
        return remote(acc.at[slot % 2], xbuf.at[slot % 2], x_ss.at[slot], x_rs.at[slot], partner_role)

    def own_x_copy():
        return remote(acc.at[0, other_rows], xown, x_ss.at[0], x_rs.at[0], partner_role)

    def reducer(slot):
        return {1: chip, 2: 1, 3: 0}[slot]

    def sum_copy(slot, h):
        b = {1: 1 - chip, 2: 2, 3: 3}[slot]
        return remote(stage_ref.at[slot - 1, pl.ds(h * rows, rows)], parts_ref.at[chip], sum_ss.at[slot - 1, h], parts_rs.at[chip], 2 * b + h)

    def give(slot):
        pl.when(core != reducer(slot))(lambda: x_copy(slot).start())

    def take(slot):
        @pl.when(core == reducer(slot))
        def _():
            x_copy(slot).wait_recv()
            s = slot % 2

            def add(i, carry):
                r = pl.ds(pl.multiple_of(i * 64, 64), 64)
                acc[s, r] = acc[s, r] + xbuf[s, r]
                return carry

            lax.fori_loop(0, block // 64, add, 0)
            store = pltpu.make_async_copy(acc.at[s], stage_ref.at[slot - 1], out_sem)
            store.start()
            store.wait()
            for h in range(2):
                sum_copy(slot, h).start()

        pl.when(core != reducer(slot))(lambda: x_copy(slot).wait_send())

    def forward(r_from, r_to, b, kind):
        @pl.when(role == r_from)
        def _():
            tok_copy(b, r_to, kind).wait_recv()
            tok_copy(b, r_to, kind).start()

    def arrive(r, b):
        on(r, lambda: tok_copy(b, r, 1).wait_recv())

    def experts(hs):
        slot = hs // 2
        s = slot % 2
        late = slot // 2
        blk = late * slot + (1 - late) * ((chip + slot) % 2)
        mix_rows = pl.ds(pl.multiple_of(blk * block, block), block)

        def one_expert(ee, carry):
            e = (hs % 2) * (n_exp // 2) + ee
            lane = lax.broadcasted_iota(jnp.int32, (block, 128), 1)
            col = jnp.sum(jnp.where(lane == e, mix_ref[mix_rows, :], 0.0), axis=1, keepdims=True)
            wcol[...] = jnp.broadcast_to(col, (block, 128))

            @pl.when(e == 0)
            def _():
                def clear(i, c):
                    r = pl.ds(pl.multiple_of(i * 64, 64), 64)
                    acc[s, r] = jnp.zeros((64, width), jnp.float32)
                    return c

                lax.fori_loop(0, block // 64, clear, 0)

            def up_step(j, c):
                q = (slot * n_exp + e) * g_steps + j
                b = q % 2
                for cp in g_copy(q):
                    cp.wait()

                @pl.when(q + 1 < g_total)
                def _():
                    for cp in g_copy(q + 1):
                        cp.start()

                def part(n, c2):
                    cols = pl.ds(pl.multiple_of(n * 256, 256), 256)
                    zg = jnp.dot(tok[blk], gbuf[b, :, cols], preferred_element_type=jnp.float32)
                    zu = jnp.dot(tok[blk], ubuf[b, :, cols], preferred_element_type=jnp.float32)
                    a = (zg * jax.nn.sigmoid(zg) * zu).astype(jnp.bfloat16)
                    act[:, pl.ds(pl.multiple_of(j * g_tile + n * 256, 256), 256)] = a
                    return c2

                return lax.fori_loop(0, g_tile // 256, part, c)

            lax.fori_loop(0, g_steps, up_step, 0)

            def down_step(n, c):
                p = (slot * n_exp + e) * d_steps + n
                b = p % 2
                d_copy(p).wait()

                @pl.when(p + 1 < d_total)
                def _():
                    d_copy(p + 1).start()

                def part(m, c2):
                    cols = pl.ds(pl.multiple_of(m * 256, 256), 256)
                    o = jnp.dot(act[...], dbuf[b, :, cols], preferred_element_type=jnp.float32).astype(jnp.bfloat16)
                    w = jnp.concatenate([wcol[...], wcol[...]], axis=1)
                    out_cols = pl.ds(pl.multiple_of(n * d_tile + m * 256, 256), 256)
                    acc[s, :, out_cols] = acc[s, :, out_cols] + jnp.where(w > 0, w * o.astype(jnp.float32), 0.0)
                    return c2

                return lax.fori_loop(0, d_tile // 256, part, c)

            lax.fori_loop(0, d_steps, down_step, 0)
            return carry

        lax.fori_loop(0, n_exp // 2, one_expert, 0)

    @pl.when(chip < 2)
    def _():
        def half(hs, carry):
            @pl.when(hs == 2)
            def _():
                own_x_copy().start()
                forward(1, 0, 1, 1)
                forward(2, 3, 0, 1)
                arrive(0, 1)
                arrive(3, 0)

            @pl.when(hs == 3)
            def _():
                own_x_copy().wait_recv()

                def add(i, c):
                    r = pl.ds(pl.multiple_of(core * rows + i * 64, 64), 64)
                    acc[0, r] = acc[0, r] + xown[pl.ds(pl.multiple_of(i * 64, 64), 64)]
                    return c

                lax.fori_loop(0, rows // 64, add, 0)
                store = pltpu.make_async_copy(acc.at[0, own_rows], parts_ref.at[chip], out_sem)
                store.start()
                store.wait()
                own_x_copy().wait_send()
                forward(0, 1, 2, 1)
                forward(3, 2, 2, 1)
                forward(1, 0, 3, 1)
                forward(0, 2, 3, 0)

            @pl.when(hs == 4)
            def _():
                give(1)
                arrive(1, 2)
                arrive(2, 2)

            @pl.when(hs == 5)
            def _():
                take(1)
                forward(2, 3, 3, 1)

            @pl.when(hs == 6)
            def _():
                give(2)
                arrive(3, 3)

            pl.when(hs == 7)(lambda: take(2))
            experts(hs)
            return carry

        lax.fori_loop(0, 8, half, 0)
        give(3)
        take(3)
        for slot in (1, 2, 3):
            @pl.when(core == reducer(slot))
            def _():
                for h in range(2):
                    sum_copy(slot, h).wait_send()

    own_copy.wait_send()
    for r, b, target, kind in ((0, 0, 2, 0), (3, 1, 1, 0), (5, 2, 0, 0), (4, 2, 3, 0), (7, 3, 1, 0), (1, 1, 0, 1), (2, 0, 3, 1), (0, 2, 1, 1), (3, 2, 2, 1), (1, 3, 0, 1), (0, 3, 2, 0), (2, 3, 3, 1)):
        on(r, lambda: tok_copy(b, target, kind).wait_send())
    for k in range(2):
        @pl.when(chip != k)
        def _():
            remote(parts_ref.at[k], parts_ref.at[k], sum_ss.at[0, 0], parts_rs.at[k], partner_role).wait_recv()


def moe_layer(layer_idx, n_group, tokens, mix, gate_w, up_w, down_w):
    rows, width = tokens.shape
    n_exp, _, ff = gate_w.shape
    block = 2 * rows
    hbm = pl.BlockSpec(memory_space=pl.ANY)
    dma = pltpu.SemaphoreType.DMA
    g_tile, d_tile = ff // 3, width // 2
    flops = 2 * 8 * rows * n_exp * 3 * width * ff
    parts, _ = pl.pallas_call(
        functools.partial(moe_body, layer_idx, (n_group, rows, width, ff, n_exp)),
        out_shape=(jax.ShapeDtypeStruct((2, rows, width), jnp.float32), jax.ShapeDtypeStruct((3, block, width), jnp.float32)),
        in_specs=[hbm, pl.BlockSpec(memory_space=pltpu.VMEM), hbm, hbm, hbm],
        out_specs=(hbm, hbm),
        scratch_shapes=[
            pltpu.VMEM((4, block, width), jnp.bfloat16),
            pltpu.VMEM((2, width, g_tile), jnp.bfloat16),
            pltpu.VMEM((2, width, g_tile), jnp.bfloat16),
            pltpu.VMEM((2, ff, d_tile), jnp.bfloat16),
            pltpu.VMEM((block, ff), jnp.bfloat16),
            pltpu.VMEM((2, block, width), jnp.float32),
            pltpu.VMEM((2, block, width), jnp.float32),
            pltpu.VMEM((rows, width), jnp.float32),
            pltpu.VMEM((block, 128), jnp.float32),
            dma, dma, dma((2,)), dma((2,)), dma((2,)), dma, dma, dma((2, 4)), dma((4,)), dma((4,)), dma((4,)), dma((3, 2)), dma((2,)),
        ],
        compiler_params=pltpu.CompilerParams(has_side_effects=True, vmem_limit_bytes=64 * 1000 * 1000),
        cost_estimate=pl.CostEstimate(flops=flops, bytes_accessed=4 * 3 * n_exp * width * ff * 2, transcendentals=0),
    )(tokens, mix, gate_w, up_w, down_w)
    return parts


def solution(mesh):
    n_stage = mesh.shape["stage"]
    n_group = mesh.shape["expert"]

    def per_device(gate_loc, up_loc, down_loc, x_loc, ids_loc, mix_loc):
        group_idx = lax.axis_index("expert")
        weights = (gate_loc[0], up_loc[0], down_loc[0])
        exp_loc = gate_loc.shape[1]
        exp_dev = exp_loc // n_stage
        n_experts = exp_loc * n_group
        chosen = ids_loc[..., None] == jnp.arange(n_experts)[None, None, None, :]
        dense_mix = jnp.sum(jnp.where(chosen, mix_loc[..., None], 0.0), axis=2)
        all_mix = lax.all_gather(dense_mix, FLAT, axis=0)
        hidden = x_loc.astype(jnp.float32)
        normed = norm_rows(hidden)
        chunks = []
        layer_outs = []
        for layer_idx in range(n_stage):
            meta = round_meta(layer_idx, n_stage, n_group)
            meta, all_mix, normed = lax.optimization_barrier((meta, all_mix, normed))
            chunks += send_round(layer_idx, meta, *weights, n_stage, n_group)
            layer_mix = all_mix[:, layer_idx]
            layer_mix = layer_mix[::-1] if layer_idx else layer_mix
            mine = lax.dynamic_slice_in_dim(layer_mix.reshape(-1, n_experts), group_idx * exp_loc, exp_loc, axis=1)
            mine = jnp.pad(mine, ((0, 0), (0, 128 - exp_loc)))
            parts = moe_layer(layer_idx, n_group, normed, mine, *weights)
            hidden = hidden + (parts[0] + parts[1])
            normed = norm_rows(hidden)
            layer_outs.append(hidden)
        outs = {"w13": None, "down": None}
        shapes = {"w13": (n_stage, exp_dev, gate_loc.shape[2], 2 * gate_loc.shape[3]), "down": (n_stage, exp_dev) + down_loc.shape[2:]}
        metas = [round_meta(r, n_stage, n_group) for r in range(n_stage)]
        for idx, kind, row_start, own, landed in chunks:
            outs[kind] = place(outs[kind], landed, own, metas[idx // (len(chunks) // n_stage)], shapes[kind], row_start)
        return outs["w13"], outs["down"], jnp.stack(layer_outs)

    weight_spec = P("stage", "expert")
    token_spec = P(None, FLAT)
    return jax.shard_map(per_device, mesh=mesh, in_specs=(weight_spec, weight_spec, weight_spec, P(FLAT), token_spec, token_spec), out_specs=(token_spec, token_spec, token_spec), check_vma=False)
```

```python
import functools

import jax
import jax.numpy as jnp
from jax import lax
from jax.experimental import pallas as pl
from jax.experimental.pallas import tpu as pltpu
from jax.sharding import PartitionSpec as P


NORM_EPS = 1e-6
FLAT = ("stage", "expert")
W13_CHUNKS = 4
DOWN_CHUNKS = 2


def norm_rows(hidden):
    return (hidden * lax.rsqrt(jnp.mean(hidden * hidden, axis=-1, keepdims=True) + NORM_EPS)).astype(jnp.bfloat16)


def copy_through(moves):
    for loads, _ in moves:
        for cp in loads:
            cp.start()
    for loads, store in moves:
        for cp in loads:
            cp.wait()
        store.start()
    for _, store in moves:
        store.wait()


def pick_w13_body(row_start, n, meta_ref, gate_ref, up_ref, out_ref, buf, sem_in, sem_out):
    exp_dev, rows, width = out_ref.shape
    half = width // 2
    tile = rows // n
    moves = []
    for e in range(exp_dev):
        for i in range(n):
            k = e * n + i
            src = pl.ds(row_start + i * tile, tile)
            exp = meta_ref[2] * exp_dev + e
            loads = [pltpu.make_async_copy(gate_ref.at[exp, src], buf.at[k, :, pl.ds(0, half)], sem_in.at[k, 0]),
                     pltpu.make_async_copy(up_ref.at[exp, src], buf.at[k, :, pl.ds(half, half)], sem_in.at[k, 1])]
            moves.append((loads, pltpu.make_async_copy(buf.at[k], out_ref.at[e, pl.ds(i * tile, tile)], sem_out.at[k])))
    copy_through(moves)


def pick_down_body(row_start, n, meta_ref, down_ref, out_ref, buf, sem_in, sem_out):
    exp_dev, rows, _ = out_ref.shape
    tile = rows // n
    moves = []
    for e in range(exp_dev):
        for i in range(n):
            k = e * n + i
            src = pl.ds(row_start + i * tile, tile)
            loads = [pltpu.make_async_copy(down_ref.at[meta_ref[2] * exp_dev + e, src], buf.at[k], sem_in.at[k, 0])]
            moves.append((loads, pltpu.make_async_copy(buf.at[k], out_ref.at[e, pl.ds(i * tile, tile)], sem_out.at[k])))
    copy_through(moves)


def place_body(row_start, n, meta_ref, landed_ref, own_ref, *rest):
    out_ref, buf, sem_in, sem_out = rest[-4:]
    exp_dev, rows, _ = landed_ref.shape
    tile = rows // n

    def moves_from(src_ref):
        moves = []
        for e in range(exp_dev):
            for i in range(n):
                k = e * n + i
                loads = [pltpu.make_async_copy(src_ref.at[e, pl.ds(i * tile, tile)], buf.at[k], sem_in.at[k])]
                moves.append((loads, pltpu.make_async_copy(buf.at[k], out_ref.at[meta_ref[0], e, pl.ds(row_start + i * tile, tile)], sem_out.at[k])))
        return moves

    pl.when(meta_ref[1] == 0)(lambda: copy_through(moves_from(landed_ref)))
    pl.when(meta_ref[1] != 0)(lambda: copy_through(moves_from(own_ref)))


HBM_SPEC = pl.BlockSpec(memory_space=pl.ANY)
SMEM_SPEC = pl.BlockSpec(memory_space=pltpu.SMEM)
COPY_COST = pl.CostEstimate(flops=5_000_000_000, bytes_accessed=16_000_000, transcendentals=0)
PIECES = 4


def pick(body, meta, sources, exp_dev, row_start, rows, width):
    dtype = sources[0].dtype
    n = PIECES
    return pl.pallas_call(
        functools.partial(body, row_start, n),
        out_shape=jax.ShapeDtypeStruct((exp_dev, rows, width), dtype),
        in_specs=[SMEM_SPEC] + [HBM_SPEC] * len(sources),
        out_specs=HBM_SPEC,
        scratch_shapes=[pltpu.VMEM((exp_dev * n, rows // n, width), dtype), pltpu.SemaphoreType.DMA((exp_dev * n, 2)), pltpu.SemaphoreType.DMA((exp_dev * n,))],
        cost_estimate=COPY_COST,
    )(meta, *sources)


def place(buffer, landed, own, meta, out_shape, row_start):
    exp_dev, rows, width = landed.shape
    n = PIECES
    args = [meta, landed, own] + ([] if buffer is None else [buffer])
    return pl.pallas_call(
        functools.partial(place_body, row_start, n),
        out_shape=jax.ShapeDtypeStruct(out_shape, landed.dtype),
        in_specs=[SMEM_SPEC] + [HBM_SPEC] * (len(args) - 1),
        out_specs=HBM_SPEC,
        scratch_shapes=[pltpu.VMEM((exp_dev * n, rows // n, width), landed.dtype), pltpu.SemaphoreType.DMA((exp_dev * n,)), pltpu.SemaphoreType.DMA((exp_dev * n,))],
        input_output_aliases={} if buffer is None else {3: 0},
        cost_estimate=COPY_COST,
    )(*args)


def round_meta(round_idx, n_stage, n_group):
    stage_idx = lax.axis_index("stage")
    group = lax.axis_index("expert")
    flat_idx = stage_idx * n_group + group
    piece = (stage_idx + round_idx) % n_stage
    is_self = group * n_stage + piece == flat_idx
    return jnp.stack([(flat_idx % n_stage - round_idx) % n_stage, is_self.astype(jnp.int32), piece]).astype(jnp.int32)


def send_round(round_idx, meta, gate_loc, up_loc, down_loc, n_stage, n_group):
    exp_dev = gate_loc.shape[0] // n_stage
    model_width, expert_width = gate_loc.shape[1:]
    pairs = [(s * n_group + g, g * n_stage + (s + round_idx) % n_stage) for s in range(n_stage) for g in range(n_group)]
    pairs = [p for p in pairs if p[0] != p[1]]
    chunks = []
    for kind, total, parts, width, body, sources in (
        ("w13", model_width, W13_CHUNKS, 2 * expert_width, pick_w13_body, (gate_loc, up_loc)),
        ("down", expert_width, DOWN_CHUNKS, model_width, pick_down_body, (down_loc,)),
    ):
        rows = total // parts
        for c in range(parts):
            idx = round_idx * (W13_CHUNKS + DOWN_CHUNKS) + len(chunks)
            own = pick(body, meta, sources, exp_dev, c * rows, rows, width)
            landed = lax.ppermute(own, FLAT, pairs)
            chunks.append((idx, kind, c * rows, own, landed))
    return chunks


def moe_body(layer_idx, dims, u_ref, mix_ref, gate_ref, up_ref, down_ref, parts_ref, stage_ref, tok, gbuf, ubuf, dbuf, act, acc, xbuf, xown, wcol, ld_sem, out_sem, g_sem, u_sem, d_sem, own_ss, own_rs, tok_ss, tok_rs, x_ss, x_rs, sum_ss, parts_rs, spare_ss, spare_rs):
    n_group, rows, width, ff, n_exp = dims
    block = 2 * rows
    g_tile = gbuf.shape[2]
    d_tile = dbuf.shape[2]
    g_steps = ff // g_tile
    d_steps = width // d_tile
    last = 2 * n_group - 1
    flat = lax.axis_index("stage") * n_group + lax.axis_index("expert")
    role = flat if layer_idx == 0 else last - flat
    chip = role // 2
    core = role % 2
    partner_role = 2 * chip + 1 - core

    def device(r):
        f = r if layer_idx == 0 else last - r
        return (f // n_group, f % n_group)

    def remote(src, dst, ss, rs, target):
        return pltpu.make_async_remote_copy(src_ref=src, dst_ref=dst, send_sem=ss, recv_sem=rs, device_id=device(target), device_id_type=pl.DeviceIdType.MESH)

    def tok_copy(b, target, kind):
        return remote(tok.at[b], tok.at[b], tok_ss.at[kind, b], tok_rs.at[b], target)

    def on(r, fn):
        pl.when(role == r)(fn)

    own_rows = pl.ds(pl.multiple_of(core * rows, rows), rows)
    other_rows = pl.ds(pl.multiple_of((1 - core) * rows, rows), rows)
    load_own = pltpu.make_async_copy(u_ref, tok.at[chip, own_rows], ld_sem)
    load_own.start()

    def g_copy(q):
        e, j, b = (q // g_steps) % n_exp, q % g_steps, q % 2
        cols = pl.ds(pl.multiple_of(j * g_tile, g_tile), g_tile)
        return (pltpu.make_async_copy(gate_ref.at[e, :, cols], gbuf.at[b], g_sem.at[b]),
                pltpu.make_async_copy(up_ref.at[e, :, cols], ubuf.at[b], u_sem.at[b]))

    def d_copy(p):
        e, n, b = (p // d_steps) % n_exp, p % d_steps, p % 2
        cols = pl.ds(pl.multiple_of(n * d_tile, d_tile), d_tile)
        return pltpu.make_async_copy(down_ref.at[e, :, cols], dbuf.at[b], d_sem.at[b])

    g_total = 4 * n_exp * g_steps
    d_total = 4 * n_exp * d_steps

    @pl.when(chip < 2)
    def _():
        for c in g_copy(0):
            c.start()
        d_copy(0).start()

    load_own.wait()
    own_copy = remote(tok.at[chip, own_rows], tok.at[chip, own_rows], own_ss, own_rs, partner_role)
    own_copy.start()
    own_copy.wait_recv()
    on(0, lambda: tok_copy(0, 2, 0).start())
    on(3, lambda: tok_copy(1, 1, 0).start())
    on(5, lambda: tok_copy(2, 0, 0).start())
    on(4, lambda: tok_copy(2, 3, 0).start())
    on(7, lambda: tok_copy(3, 1, 0).start())

    def x_copy(slot):
        return remote(acc.at[slot % 2], xbuf.at[slot % 2], x_ss.at[slot], x_rs.at[slot], partner_role)

    def own_x_copy():
        return remote(acc.at[0, other_rows], xown, x_ss.at[0], x_rs.at[0], partner_role)

    def reducer(slot):
        return {1: 1, 2: chip, 3: 0}[slot]

    def sum_copy(slot, h):
        b = {1: 2, 2: 1 - chip, 3: 3}[slot]
        return remote(stage_ref.at[slot - 1, pl.ds(h * rows, rows)], parts_ref.at[chip], sum_ss.at[slot - 1, h], parts_rs.at[chip], 2 * b + h)

    def spare_copy():
        return remote(stage_ref.at[1, pl.ds(0, rows)], xbuf.at[0, pl.ds(0, rows)], spare_ss, spare_rs, 1)

    def give(slot):
        pl.when(core != reducer(slot))(lambda: x_copy(slot).start())

    def take(slot):
        @pl.when(core == reducer(slot))
        def _():
            x_copy(slot).wait_recv()
            s = slot % 2

            def add(i, carry):
                r = pl.ds(pl.multiple_of(i * 64, 64), 64)
                acc[s, r] = acc[s, r] + xbuf[s, r]
                return carry

            lax.fori_loop(0, block // 64, add, 0)
            store = pltpu.make_async_copy(acc.at[s], stage_ref.at[slot - 1], out_sem)
            store.start()
            store.wait()
            for h in range(2):
                sum_copy(slot, h).start()

        pl.when(core != reducer(slot))(lambda: x_copy(slot).wait_send())

    def forward(r_from, r_to, b, kind):
        @pl.when(role == r_from)
        def _():
            tok_copy(b, r_to, kind).wait_recv()
            tok_copy(b, r_to, kind).start()

    def arrive(r, b):
        on(r, lambda: tok_copy(b, r, 1).wait_recv())

    def experts(step):
        slot = step // n_exp
        s = slot % 2
        blk = jnp.where(slot == 0, chip, jnp.where(slot == 1, 2, jnp.where(slot == 2, 1 - chip, 3)))
        mix_rows = pl.ds(pl.multiple_of(blk * block, block), block)

        def one_expert():
            e = step % n_exp
            lane = lax.broadcasted_iota(jnp.int32, (block, 128), 1)
            col = jnp.sum(jnp.where(lane == e, mix_ref[mix_rows, :], 0.0), axis=1, keepdims=True)
            wcol[...] = jnp.broadcast_to(col, (block, 128))

            @pl.when(e == 0)
            def _():
                def clear(i, c):
                    r = pl.ds(pl.multiple_of(i * 64, 64), 64)
                    acc[s, r] = jnp.zeros((64, width), jnp.float32)
                    return c

                lax.fori_loop(0, block // 64, clear, 0)

            def up_step(j, c):
                q = (slot * n_exp + e) * g_steps + j
                b = q % 2
                for cp in g_copy(q):
                    cp.wait()

                @pl.when(q + 1 < g_total)
                def _():
                    for cp in g_copy(q + 1):
                        cp.start()

                def part(n, c2):
                    cols = pl.ds(pl.multiple_of(n * 256, 256), 256)
                    zg = jnp.dot(tok[blk], gbuf[b, :, cols], preferred_element_type=jnp.float32)
                    zu = jnp.dot(tok[blk], ubuf[b, :, cols], preferred_element_type=jnp.float32)
                    a = (zg * jax.nn.sigmoid(zg) * zu).astype(jnp.bfloat16)
                    act[:, pl.ds(pl.multiple_of(j * g_tile + n * 256, 256), 256)] = a
                    return c2

                return lax.fori_loop(0, g_tile // 256, part, c)

            lax.fori_loop(0, g_steps, up_step, 0)

            def down_step(n, c):
                p = (slot * n_exp + e) * d_steps + n
                b = p % 2
                d_copy(p).wait()

                @pl.when(p + 1 < d_total)
                def _():
                    d_copy(p + 1).start()

                def part(m, c2):
                    cols = pl.ds(pl.multiple_of(m * 256, 256), 256)
                    o = jnp.dot(act[...], dbuf[b, :, cols], preferred_element_type=jnp.float32).astype(jnp.bfloat16)
                    w = jnp.concatenate([wcol[...], wcol[...]], axis=1)
                    out_cols = pl.ds(pl.multiple_of(n * d_tile + m * 256, 256), 256)
                    acc[s, :, out_cols] = acc[s, :, out_cols] + jnp.where(w > 0, w * o.astype(jnp.float32), 0.0)
                    return c2

                return lax.fori_loop(0, d_tile // 256, part, c)

            lax.fori_loop(0, d_steps, down_step, 0)

        one_expert()

    @pl.when(chip < 2)
    def _():
        def step_body(step, carry):
            @pl.when(step == n_exp)
            def _():
                own_x_copy().start()
                forward(0, 1, 2, 1)
                forward(3, 2, 2, 1)
                arrive(1, 2)
                arrive(2, 2)

            @pl.when(step == n_exp + 1)
            def _():
                own_x_copy().wait_recv()

                def add(i, c):
                    r = pl.ds(pl.multiple_of(core * rows + i * 64, 64), 64)
                    acc[0, r] = acc[0, r] + xown[pl.ds(pl.multiple_of(i * 64, 64), 64)]
                    return c

                lax.fori_loop(0, rows // 64, add, 0)
                store = pltpu.make_async_copy(acc.at[0, own_rows], parts_ref.at[chip], out_sem)
                store.start()
                store.wait()
                own_x_copy().wait_send()
                forward(1, 0, 1, 1)
                forward(2, 3, 0, 1)
                forward(1, 0, 3, 1)

            pl.when(step == n_exp + 2)(lambda: forward(0, 2, 3, 0))

            @pl.when(step == 2 * n_exp)
            def _():
                give(1)
                arrive(0, 1)
                arrive(3, 0)

            pl.when(step == 2 * n_exp + 1)(lambda: take(1))
            pl.when(step == 2 * n_exp + 2)(lambda: forward(2, 3, 3, 1))

            @pl.when(step == 3 * n_exp)
            def _():
                give(2)
                arrive(3, 3)

            @pl.when(step == 3 * n_exp + 1)
            def _():
                take(2)
                on(3, lambda: spare_copy().start())

            experts(step)
            return carry

        lax.fori_loop(0, 4 * n_exp, step_body, 0)
        give(3)
        take(3)
        on(3, lambda: spare_copy().wait_send())
        on(1, lambda: spare_copy().wait_recv())
        for slot in (1, 2, 3):
            @pl.when(core == reducer(slot))
            def _():
                for h in range(2):
                    sum_copy(slot, h).wait_send()

    own_copy.wait_send()
    for r, b, target, kind in ((0, 0, 2, 0), (3, 1, 1, 0), (5, 2, 0, 0), (4, 2, 3, 0), (7, 3, 1, 0), (1, 1, 0, 1), (2, 0, 3, 1), (0, 2, 1, 1), (3, 2, 2, 1), (1, 3, 0, 1), (0, 3, 2, 0), (2, 3, 3, 1)):
        on(r, lambda: tok_copy(b, target, kind).wait_send())
    for k in range(2):
        @pl.when(chip != k)
        def _():
            remote(parts_ref.at[k], parts_ref.at[k], sum_ss.at[0, 0], parts_rs.at[k], partner_role).wait_recv()


def moe_layer(layer_idx, n_group, tokens, mix, gate_w, up_w, down_w):
    rows, width = tokens.shape
    n_exp, _, ff = gate_w.shape
    block = 2 * rows
    hbm = pl.BlockSpec(memory_space=pl.ANY)
    dma = pltpu.SemaphoreType.DMA
    g_tile, d_tile = ff // 3, width // 2
    flops = 2 * 8 * rows * n_exp * 3 * width * ff
    parts, _ = pl.pallas_call(
        functools.partial(moe_body, layer_idx, (n_group, rows, width, ff, n_exp)),
        out_shape=(jax.ShapeDtypeStruct((2, rows, width), jnp.float32), jax.ShapeDtypeStruct((3, block, width), jnp.float32)),
        in_specs=[hbm, pl.BlockSpec(memory_space=pltpu.VMEM), hbm, hbm, hbm],
        out_specs=(hbm, hbm),
        scratch_shapes=[
            pltpu.VMEM((4, block, width), jnp.bfloat16),
            pltpu.VMEM((2, width, g_tile), jnp.bfloat16),
            pltpu.VMEM((2, width, g_tile), jnp.bfloat16),
            pltpu.VMEM((2, ff, d_tile), jnp.bfloat16),
            pltpu.VMEM((block, ff), jnp.bfloat16),
            pltpu.VMEM((2, block, width), jnp.float32),
            pltpu.VMEM((2, block, width), jnp.float32),
            pltpu.VMEM((rows, width), jnp.float32),
            pltpu.VMEM((block, 128), jnp.float32),
            dma, dma, dma((2,)), dma((2,)), dma((2,)), dma, dma, dma((2, 4)), dma((4,)), dma((4,)), dma((4,)), dma((3, 2)), dma((2,)), dma, dma,
        ],
        compiler_params=pltpu.CompilerParams(has_side_effects=True, vmem_limit_bytes=64 * 1000 * 1000),
        cost_estimate=pl.CostEstimate(flops=flops, bytes_accessed=4 * 3 * n_exp * width * ff * 2, transcendentals=0),
    )(tokens, mix, gate_w, up_w, down_w)
    return parts


def solution(mesh):
    n_stage = mesh.shape["stage"]
    n_group = mesh.shape["expert"]

    def per_device(gate_loc, up_loc, down_loc, x_loc, ids_loc, mix_loc):
        group_idx = lax.axis_index("expert")
        weights = (gate_loc[0], up_loc[0], down_loc[0])
        exp_loc = gate_loc.shape[1]
        exp_dev = exp_loc // n_stage
        n_experts = exp_loc * n_group
        chosen = ids_loc[..., None] == jnp.arange(n_experts)[None, None, None, :]
        dense_mix = jnp.sum(jnp.where(chosen, mix_loc[..., None], 0.0), axis=2)
        all_mix = lax.all_gather(dense_mix, FLAT, axis=0)
        hidden = x_loc.astype(jnp.float32)
        normed = norm_rows(hidden)
        chunks = []
        layer_outs = []
        for layer_idx in range(n_stage):
            if layer_idx == 0:
                for r in range(n_stage):
                    meta, all_mix, normed = lax.optimization_barrier((round_meta(r, n_stage, n_group), all_mix, normed))
                    chunks += send_round(r, meta, *weights, n_stage, n_group)
            layer_mix = all_mix[:, layer_idx]
            layer_mix = layer_mix[::-1] if layer_idx else layer_mix
            mine = lax.dynamic_slice_in_dim(layer_mix.reshape(-1, n_experts), group_idx * exp_loc, exp_loc, axis=1)
            mine = jnp.pad(mine, ((0, 0), (0, 128 - exp_loc)))
            parts = moe_layer(layer_idx, n_group, normed, mine, *weights)
            hidden = hidden + (parts[0] + parts[1])
            normed = norm_rows(hidden)
            layer_outs.append(hidden)
        outs = {"w13": None, "down": None}
        shapes = {"w13": (n_stage, exp_dev, gate_loc.shape[2], 2 * gate_loc.shape[3]), "down": (n_stage, exp_dev) + down_loc.shape[2:]}
        metas = [round_meta(r, n_stage, n_group) for r in range(n_stage)]
        for idx, kind, row_start, own, landed in chunks:
            outs[kind] = place(outs[kind], landed, own, metas[idx // (len(chunks) // n_stage)], shapes[kind], row_start)
        return outs["w13"], outs["down"], jnp.stack(layer_outs)

    weight_spec = P("stage", "expert")
    token_spec = P(None, FLAT)
    return jax.shard_map(per_device, mesh=mesh, in_specs=(weight_spec, weight_spec, weight_spec, P(FLAT), token_spec, token_spec), out_specs=(token_spec, token_spec, token_spec), check_vma=False)
```
